256 devices in a mesh: batch: 128 (over x_hi, y, z, core), rep: 2 (over x_lo).
Axes of the slice: x: 4 (x_hi: 2, x_lo: 2; x = x_hi * 2 + x_lo), y: 4, z: 8, core: 2. Of those that a mesh axis runs over, the one named last changes fastest.
Arguments:
- image_embed: bfloat16 [16384, 1024], P('batch'), may hold values from -2 to 2
- text_embed: bfloat16 [16384, 1024], P(('batch', 'rep')), may hold values from -2 to 2
- logit_scale: float32 [1], replicated, may hold values from 50 to 100
Outputs:
- mean_loss: float32 [], replicated
- image_grad: float32 [16384, 1024], P(('batch', 'rep'))
- text_grad: float32 [16384, 1024], P(('batch', 'rep'))
The draws below stay inside these ranges and needn't reach their ends.
All inputs are finite; a program needn't handle non-finite values.
Results may differ from the reference program's by a relative error of at most 0.0025.
Values may be sent and summed in bfloat16 or wider, within the bound.
No kernel may reach another device: no remote copies, remote signals or barrier semaphores. Data moves between devices by JAX's collectives and lax.ppermute only.
A program may use at most 128 MiB of HBM per device.

```python
import math
import jax
import jax.numpy as jnp
from jax import lax

D = 1024
PAIRS = 16384


def pair_draw(key):
    base_key = jax.random.fold_in(key, 17)
    keys = jax.random.split(base_key, 2)
    text_rows = jax.random.normal(keys[0], (PAIRS, D), jnp.float32) * D ** (-0.5)
    image_rows = jax.random.normal(keys[1], (PAIRS, D), jnp.float32) * D ** (-0.5)
    return (jnp.clip(image_rows, -2.0, 2.0), jnp.clip(text_rows, -2.0, 2.0))


def draw_image_embed(key, part):
    return pair_draw(key)[0].astype(jnp.bfloat16)


def draw_text_embed(key, part):
    return pair_draw(key)[1].astype(jnp.bfloat16)


def setup_inputs(seed: int = 0) -> dict:
    seeds = jax.random.split(jax.random.key(seed), 4)
    image_embed = draw_image_embed(jax.random.fold_in(seeds[3], 71), 0)
    text_embed = draw_text_embed(jax.random.fold_in(seeds[3], 71), 0)
    logit_scale = jnp.clip(jnp.exp(jax.random.uniform(seeds[2], (1,), jnp.float32, math.log(50.0), math.log(100.0))), 50.0, 100.0)
    return {"image_embed": image_embed, "text_embed": text_embed, "logit_scale": logit_scale}


def scores_of(left_rows, right_rows, scale_value):
    return scale_value * lax.dot_general(left_rows, right_rows, (((1,), (1,)), ((), ())), preferred_element_type=jnp.float32)


def reference(image_embed, text_embed, logit_scale):
    scale_value = logit_scale[0]
    block_rows = math.gcd(PAIRS, 1024)
    block_count = PAIRS // block_rows
    starts = (jnp.arange(block_count) * block_rows).astype(jnp.int32)

    def lse_rows(first_row, mine, other):
        picked = lax.dynamic_slice_in_dim(mine, first_row, block_rows, 0)
        scores = scores_of(picked, other, scale_value)
        biggest = jnp.max(scores, axis=1)
        return biggest + jnp.log(jnp.sum(jnp.exp(scores - biggest[:, None]), axis=1))

    row_lse = lax.map(lambda first_row: lse_rows(first_row, image_embed, text_embed), starts).reshape(PAIRS)
    col_lse = lax.map(lambda first_row: lse_rows(first_row, text_embed, image_embed), starts).reshape(PAIRS)
    diagonal = scale_value * jnp.sum(image_embed.astype(jnp.float32) * text_embed.astype(jnp.float32), axis=1)
    mean_loss = jnp.sum(row_lse + col_lse - 2.0 * diagonal) / (2 * PAIRS)

    def grad_rows(first_row, mine, other, mine_lse, other_lse):
        picked = lax.dynamic_slice_in_dim(mine, first_row, block_rows, 0)
        picked_lse = lax.dynamic_slice_in_dim(mine_lse, first_row, block_rows, 0)
        scores = scores_of(picked, other, scale_value)
        row_ids = first_row + lax.broadcasted_iota(jnp.int32, scores.shape, 0)
        column_ids = lax.broadcasted_iota(jnp.int32, scores.shape, 1)
        match = (row_ids == column_ids).astype(jnp.float32)
        weights = (jnp.exp(scores - picked_lse[:, None]) + jnp.exp(scores - other_lse[None, :]) - 2.0 * match).astype(jnp.bfloat16)
        return (scale_value * 0.5) * jnp.dot(weights, other, preferred_element_type=jnp.float32)

    image_grad = lax.map(lambda first_row: grad_rows(first_row, image_embed, text_embed, row_lse, col_lse), starts).reshape(PAIRS, D)
    text_grad = lax.map(lambda first_row: grad_rows(first_row, text_embed, image_embed, col_lse, row_lse), starts).reshape(PAIRS, D)
    return (mean_loss, image_grad, text_grad)
```

```python
import jax
import jax.numpy as jnp
from jax import lax
from jax.sharding import Mesh
from jax.sharding import PartitionSpec as P

BATCH = ("xh", "y", "z", "c")
BATCH_REP = ("xh", "y", "z", "c", "xl")
PLANE = ("xh", "y", "xl")
LINE = ("z", "c")
WIRE_SCALE = 8.0


def to_each(array, axis):
    peers = lax.axis_size(axis)
    return lax.all_to_all(
        jnp.broadcast_to(array[None], (peers, *array.shape)), axis, 0, 0, tiled=True
    )


def shifted(array, axis, by):
    peers = lax.axis_size(axis)
    return lax.ppermute(array, axis, [(k, (k + by) % peers) for k in range(peers)])


def swapped(array):
    return lax.ppermute(array, "c", [(0, 1), (1, 0)])


def lse_of(scores, axis):
    biggest = jnp.max(scores, axis=axis, keepdims=True)
    total = jnp.sum(jnp.exp(scores - biggest), axis=axis)
    return jnp.squeeze(biggest, axis) + jnp.log(total)


def body(image_embed, text_embed, logit_scale):
    scale_value = logit_scale[0]
    rows = text_embed.shape[0]
    line = lax.axis_size("z")
    plane = lax.axis_size(PLANE)
    core = lax.axis_index("c")
    own_image = lax.dynamic_slice_in_dim(image_embed, lax.axis_index("xl") * rows, rows, 0)
    own_diag = scale_value * jnp.sum(
        own_image.astype(jnp.float32) * text_embed.astype(jnp.float32)
    )

    text_all = to_each(text_embed, PLANE).reshape(plane * rows, -1)
    near = jnp.concatenate([own_image] + [shifted(own_image, "z", k) for k in range(1, line)])
    image_all = jnp.concatenate([near, swapped(near)])
    half = line * rows
    scores = scale_value * lax.dot_general(
        image_all, text_all, (((1,), (1,)), ((), ())), preferred_element_type=jnp.float32
    )

    def by_place(halves):
        return jnp.where(core == 0, halves, halves[::-1])

    z_index = lax.axis_index("z")
    part_rows = lse_of(scores, 1).reshape(2, line, rows)
    slots = (z_index - jnp.arange(line)) % line
    placed_rows = by_place(part_rows[:, slots])
    message = jnp.concatenate(
        [placed_rows.reshape(-1), jnp.broadcast_to(own_diag, (128,))]
    ).reshape(1, -1)
    heard = to_each(message, LINE).reshape(2 * line, -1)
    all_rows = lse_of(heard[:, : 2 * half], 0)
    row_total = jnp.sum(all_rows) - 2.0 * jnp.sum(heard[:, 2 * half])
    row_lse = by_place(all_rows.reshape(2, line, rows))[:, slots].reshape(-1)

    part_cols = lse_of(scores, 0)
    message = jnp.concatenate([part_cols, jnp.broadcast_to(row_total, (128,))]).reshape(1, -1)
    heard = to_each(message, PLANE).reshape(plane, -1)
    col_lse = lse_of(heard[:, : plane * rows], 0)
    rows_loss = jnp.sum(heard[:, plane * rows])
    cols_loss = jnp.sum(to_each(jnp.broadcast_to(jnp.sum(col_lse), (1, 128)), LINE)[:, 0, 0])
    mean_loss = (rows_loss + cols_loss) / (2 * 2 * line * plane * rows)

    row_ids = lax.broadcasted_iota(jnp.int32, scores.shape, 0)
    column_ids = lax.broadcasted_iota(jnp.int32, scores.shape, 1) - lax.axis_index(PLANE) * rows
    match = ((row_ids == column_ids) & (row_ids < rows)).astype(jnp.float32)
    weights = (
        jnp.exp(scores - row_lse[:, None]) + jnp.exp(scores - col_lse[None, :]) - 2.0 * match
    ).astype(jnp.bfloat16)

    other = jnp.dot(weights[half:], text_all, preferred_element_type=jnp.float32)
    other = swapped((WIRE_SCALE * other).astype(jnp.float16)).astype(jnp.float32)
    text_part = lax.dot_general(
        weights, image_all, (((0,), (0,)), ((), ())), preferred_element_type=jnp.float32
    )
    text_part = (WIRE_SCALE * text_part).astype(jnp.float16).reshape(plane, rows, -1)
    text_sum = lax.all_to_all(text_part, PLANE, 0, 0, tiled=True).astype(jnp.float32).sum(axis=0)
    near_part = WIRE_SCALE * jnp.dot(weights[:half], text_all, preferred_element_type=jnp.float32)
    near_part = (near_part + other).reshape(line, rows, -1)
    image_sum = near_part[0]
    for k in range(1, line):
        image_sum = image_sum + shifted(near_part[k].astype(jnp.float16), "z", -k).astype(
            jnp.float32
        )
    factor = scale_value * (0.5 / WIRE_SCALE)
    return (mean_loss, factor * image_sum, factor * text_sum)


def solution(mesh):
    split = Mesh(
        mesh.devices.reshape(2, 4, 8, 2, mesh.shape["rep"]),
        BATCH_REP,
    )
    return jax.shard_map(
        body,
        mesh=split,
        in_specs=(P(BATCH, None), P(BATCH_REP, None), P()),
        out_specs=(P(), P(BATCH_REP, None), P(BATCH_REP, None)),
        check_vma=False,
    )
```

```python
import jax
import jax.numpy as jnp
from jax import lax
from jax.experimental import pallas as pl
from jax.experimental.pallas import tpu as pltpu
from jax.sharding import Mesh
from jax.sharding import PartitionSpec as P


BATCH = ("xh", "y", "z", "c")
BATCH_REP = ("xh", "y", "z", "c", "xl")
PLANE = ("xh", "y", "xl")
LINE = ("z", "c")
WIRE_SCALE = 8.0
ROWS = 64
LINE_Z = 8
PLANE_N = 16
HALF = LINE_Z * ROWS
BLOCK = 2 * HALF
LANES = 128
TILES = BLOCK // LANES
STEP = 256
FAR_FIRST = (4, 3, 5, 2, 6, 1, 7)
NT = (((1,), (1,)), ((), ()))
NN = (((1,), (0,)), ((), ()))
TN = (((0,), (0,)), ((), ()))


def exchanged(message, axis):
    return lax.all_to_all(message, axis, 0, 0, tiled=True)


def shifted(array, by):
    return lax.ppermute(array, "z", [(k, (k + by) % LINE_Z) for k in range(LINE_Z)])


def swapped(array):
    return lax.ppermute(array, "c", [(0, 1), (1, 0)])


def as_column(line):
    return jnp.transpose(jnp.broadcast_to(line, (LANES, LANES)))[:ROWS, :1]


def as_line(column):
    return jnp.transpose(jnp.broadcast_to(column, (LANES, LANES)))[:1]


def placed(slots, pos):
    turned = [pltpu.roll(slots[at : at + LINE_Z], pos[1], 0) for at in (0, LINE_Z)]
    return jnp.where(
        pos[0] == 0, jnp.concatenate(turned, axis=0), jnp.concatenate(turned[::-1], axis=0)
    )


def relative(slots, pos):
    back = lax.rem(LINE_Z - pos[1], LINE_Z)
    turned = [pltpu.roll(slots[at : at + LINE_Z], back, 0) for at in (0, LINE_Z)]
    return jnp.where(
        pos[0] == 0, jnp.concatenate(turned, axis=0), jnp.concatenate(turned[::-1], axis=0)
    )


def scores_kernel(pos, scale, own_text, text, *refs):
    blocks, (scores, image, row_message, col_part) = refs[: 2 * LINE_Z], refs[2 * LINE_Z :]
    for k in range(2 * LINE_Z):
        image[k * ROWS : (k + 1) * ROWS, :] = blocks[k][...]
    scale_value = scale[0]
    diag = scale_value * jnp.sum(
        blocks[0][...].astype(jnp.float32) * own_text[...].astype(jnp.float32)
    )
    text_rows = text[...]
    col_max = col_sum = None
    lines = []
    for i in range(BLOCK // STEP):
        span = slice(i * STEP, (i + 1) * STEP)
        part = scale_value * lax.dot_general(
            image[span, :], text_rows, NT, preferred_element_type=jnp.float32
        )
        scores[span, :] = part
        biggest = jnp.max(part, axis=1, keepdims=True)
        lse = biggest + jnp.log(jnp.sum(jnp.exp(part - biggest), axis=1, keepdims=True))
        for t in range(STEP // LANES):
            line = as_line(lse[t * LANES : (t + 1) * LANES])
            lines += [line, pltpu.roll(line, ROWS, 1)]
        top = jnp.max(part, axis=0, keepdims=True)
        new = top if i == 0 else jnp.maximum(col_max, top)
        total = jnp.sum(jnp.exp(part - new), axis=0, keepdims=True)
        col_sum = total if i == 0 else col_sum * jnp.exp(col_max - new) + total
        col_max = new
    slots = placed(jnp.concatenate(lines, axis=0), pos)
    lanes = lax.broadcasted_iota(jnp.int32, slots.shape, 1)
    message = jnp.where(lanes < ROWS, slots, diag)
    row_message[...] = jnp.broadcast_to(message[None], row_message.shape)
    col_lse = col_max + jnp.log(col_sum)
    for i in range(TILES):
        col_part[i : i + 1, :] = col_lse[:, i * LANES : (i + 1) * LANES]


def joined(stats):
    biggest = jnp.max(stats, axis=0)
    return biggest + jnp.log(jnp.sum(jnp.exp(stats - biggest[None]), axis=0))


def rows_kernel(pos, heard, col_part, row_lse, col_message):
    lse = joined(heard[...])
    lanes = lax.broadcasted_iota(jnp.int32, lse.shape, 1)
    diag = jnp.sum(heard[...], axis=0)[:TILES, ROWS : ROWS + 1]
    extra = jnp.sum(jnp.where(lanes < ROWS, lse, 0.0)) - 2.0 * diag
    row_lse[...] = relative(lse, pos)
    message = jnp.concatenate([col_part[...], jnp.broadcast_to(extra, (TILES, LANES))], axis=0)
    col_message[...] = jnp.broadcast_to(message[None], col_message.shape)


def weights_kernel(pos, scores, row_lse, heard, weights, loss_message, rows_loss):
    col_lse = joined(heard[:, :TILES, :])
    rows_loss[...] = jnp.sum(heard[:, TILES:, :], axis=0)
    loss_message[...] = jnp.full(loss_message.shape, jnp.sum(col_lse))
    col_line = jnp.concatenate([col_lse[i : i + 1] for i in range(TILES)], axis=1)
    for k in range(2 * LINE_Z):
        span = slice(k * ROWS, (k + 1) * ROWS)
        part = scores[span, :]
        both = jnp.exp(part - as_column(row_lse[k : k + 1, :])) + jnp.exp(part - col_line)
        if k == 0:
            row_ids = lax.broadcasted_iota(jnp.int32, part.shape, 0)
            column_ids = lax.broadcasted_iota(jnp.int32, part.shape, 1) - pos[2] * ROWS
            both = both - 2.0 * (row_ids == column_ids).astype(jnp.float32)
        weights[span, :] = both.astype(jnp.bfloat16)


def call(kernel, outs, spec, *args):
    vmem = pl.BlockSpec(memory_space=pltpu.VMEM)
    smem = pl.BlockSpec(memory_space=pltpu.SMEM)
    return pl.pallas_call(
        kernel,
        out_shape=[jax.ShapeDtypeStruct(*o) for o in outs],
        in_specs=[smem if s == "s" else vmem for s in spec],
        out_specs=[vmem] * len(outs),
        compiler_params=pltpu.CompilerParams(vmem_limit_bytes=48 * 1024 * 1024),
    )(*args)


def parts(image_embed, text_embed, logit_scale):
    f32, f16, bf16 = jnp.float32, jnp.float16, jnp.bfloat16
    width = text_embed.shape[1]
    pos = jnp.stack(
        [lax.axis_index("c"), lax.axis_index("z"), lax.axis_index(PLANE)]
    ).astype(jnp.int32)
    own_image = lax.dynamic_slice_in_dim(image_embed, lax.axis_index("xl") * ROWS, ROWS, 0)

    text_all = exchanged(
        jnp.broadcast_to(text_embed[None], (PLANE_N, *text_embed.shape)), PLANE
    ).reshape(BLOCK, width)
    near = [own_image] + [None] * (LINE_Z - 1)
    for k in FAR_FIRST:
        near[k] = shifted(own_image, -k)
    far = [None] * LINE_Z
    for k in range(LINE_Z):
        far[k] = swapped(near[k])

    message = (PLANE_N, 2 * TILES, LANES)
    scores, image_all, row_message, col_part = call(
        scores_kernel,
        [((BLOCK, BLOCK), f32), ((BLOCK, width), bf16), (message, f32), ((TILES, LANES), f32)],
        "ss" + "v" * (2 + 2 * LINE_Z),
        pos, logit_scale, text_embed, text_all, *near, *far,
    )
    row_lse, col_message = call(
        rows_kernel,
        [((2 * LINE_Z, LANES), f32), (message, f32)],
        "svv",
        pos, exchanged(row_message, LINE), col_part,
    )
    weights, loss_message, rows_loss = call(
        weights_kernel,
        [((BLOCK, BLOCK), bf16), ((PLANE_N, TILES, LANES), f32), ((TILES, LANES), f32)],
        "svvv",
        pos, scores, row_lse, exchanged(col_message, PLANE),
    )
    heard = exchanged(loss_message, LINE)
    mean_loss = (rows_loss[0, 0] + jnp.sum(heard[:, 0, 0])) / (2 * ROWS * 256)

    other = lax.dot_general(weights[HALF:], text_all, NN, preferred_element_type=f32)
    arrived = swapped((WIRE_SCALE * other).astype(f16))
    text_part = lax.dot_general(weights, image_all, TN, preferred_element_type=f32)
    text_part = (WIRE_SCALE * text_part).astype(f16).reshape(PLANE_N, ROWS, width)
    text_sum = exchanged(text_part, PLANE).astype(f32).sum(axis=0)
    image_part = WIRE_SCALE * lax.dot_general(
        weights[:HALF], text_all, NN, preferred_element_type=f32
    ) + arrived.astype(f32)
    image_part = image_part.reshape(LINE_Z, ROWS, width)
    back = {}
    for k in FAR_FIRST:
        back[k] = shifted(image_part[k].astype(f16), k)
    image_sum = image_part[0]
    for k in range(1, LINE_Z):
        image_sum = image_sum + back[k].astype(f32)
    factor = logit_scale[0] * (0.5 / WIRE_SCALE)
    return (mean_loss, factor * image_sum, factor * text_sum)


def solution(mesh):
    split = Mesh(mesh.devices.reshape(2, 4, LINE_Z, 2, mesh.shape["rep"]), BATCH_REP)
    return jax.shard_map(
        parts,
        mesh=split,
        in_specs=(P(BATCH, None), P(BATCH_REP, None), P()),
        out_specs=(P(), P(BATCH_REP, None), P(BATCH_REP, None)),
        check_vma=False,
    )
```

```python
import jax
import jax.numpy as jnp
from jax import lax
from jax.experimental import pallas as pl
from jax.experimental.pallas import tpu as pltpu
from jax.sharding import Mesh
from jax.sharding import PartitionSpec as P


BATCH = ("xh", "y", "z", "c")
BATCH_REP = ("xh", "y", "z", "c", "xl")
PLANE = ("xh", "y", "xl")
LINE = ("z", "c")
WIRE_SCALE = 8.0
VMEM_LIMIT = 24 * 1024 * 1024
ROWS = 64
LINE_Z = 8
PLANE_N = 16
HALF = LINE_Z * ROWS
BLOCK = 2 * HALF
LANES = 128
TILES = BLOCK // LANES
STEP = 256
FAR_FIRST = (4, 3, 5, 2, 6, 1, 7)
NT = (((1,), (1,)), ((), ()))
NN = (((1,), (0,)), ((), ()))
TN = (((0,), (0,)), ((), ()))


def exchanged(message, axis):
    return lax.all_to_all(message, axis, 0, 0, tiled=True)


def shifted(array, by):
    return lax.ppermute(array, "z", [(k, (k + by) % LINE_Z) for k in range(LINE_Z)])


def swapped(array):
    return lax.ppermute(array, "c", [(0, 1), (1, 0)])


def as_column(line):
    return jnp.transpose(jnp.broadcast_to(line, (LANES, LANES)))[:ROWS, :1]


def as_line(column):
    return jnp.transpose(jnp.broadcast_to(column, (LANES, LANES)))[:1]


def placed(slots, pos):
    lanes = lax.broadcasted_iota(jnp.int32, (LINE_Z, LANES), 1)
    both = jnp.where(lanes < ROWS, slots[:LINE_Z], pltpu.roll(slots[LINE_Z:], ROWS, 1))
    return pltpu.roll(jnp.where(pos[0] == 0, both, pltpu.roll(both, ROWS, 1)), pos[1], 0)


def relative(both, pos):
    both = pltpu.roll(both, lax.rem(LINE_Z - pos[1], LINE_Z), 0)
    turned = pltpu.roll(both, ROWS, 1)
    same = pos[0] == 0
    return jnp.concatenate(
        [jnp.where(same, both, turned), jnp.where(same, turned, both)], axis=0
    )


def scores_kernel(pos, scale, own_text, text, *refs):
    blocks, rest = refs[: 2 * LINE_Z], refs[2 * LINE_Z :]
    scores, image, row_message, col_part, diag_part = rest
    for k in range(2 * LINE_Z):
        image[k * ROWS : (k + 1) * ROWS, :] = blocks[k][...]
    scale_value = scale[0]
    diag = scale_value * jnp.sum(
        blocks[0][...].astype(jnp.float32) * own_text[...].astype(jnp.float32)
    )
    text_rows = text[...]
    col_max = col_sum = None
    lines = []
    for i in range(BLOCK // STEP):
        span = slice(i * STEP, (i + 1) * STEP)
        part = scale_value * lax.dot_general(
            image[span, :], text_rows, NT, preferred_element_type=jnp.float32
        )
        scores[span, :] = part
        biggest = jnp.max(part, axis=1, keepdims=True)
        lse = biggest + jnp.log(jnp.sum(jnp.exp(part - biggest), axis=1, keepdims=True))
        for t in range(STEP // LANES):
            line = as_line(lse[t * LANES : (t + 1) * LANES])
            lines += [line, pltpu.roll(line, ROWS, 1)]
        top = jnp.max(part, axis=0, keepdims=True)
        new = top if i == 0 else jnp.maximum(col_max, top)
        total = jnp.sum(jnp.exp(part - new), axis=0, keepdims=True)
        col_sum = total if i == 0 else col_sum * jnp.exp(col_max - new) + total
        col_max = new
    message = placed(jnp.concatenate(lines, axis=0), pos)
    diag_part[...] = jnp.full(diag_part.shape, diag)
    row_message[...] = jnp.broadcast_to(message[None], row_message.shape)
    col_lse = col_max + jnp.log(col_sum)
    for i in range(TILES):
        col_part[i : i + 1, :] = col_lse[:, i * LANES : (i + 1) * LANES]


def joined(stats):
    biggest = jnp.max(stats, axis=0)
    return biggest + jnp.log(jnp.sum(jnp.exp(stats - biggest[None]), axis=0))


def rows_kernel(pos, heard, col_part, diag_part, row_lse, col_message):
    lse = joined(heard[...])
    row_lse[...] = relative(lse, pos)
    extra = lax.broadcasted_iota(jnp.int32, (TILES, LANES), 0)
    extra = jnp.where(extra == 0, jnp.sum(lse), diag_part[...])
    message = jnp.concatenate([col_part[...], extra], axis=0)
    col_message[...] = jnp.broadcast_to(message[None], col_message.shape)


def weights_kernel(pos, scores, row_lse, heard, text, weights, near, other, loss_part, rows_loss):
    step = pl.program_id(0)
    col_lse = joined(heard[:, :TILES, :])
    extra = jnp.sum(heard[:, TILES:, :], axis=0)
    rows_loss[...] = jnp.broadcast_to(extra[:1], rows_loss.shape)
    loss_part[...] = jnp.sum(col_lse) - 2.0 * jnp.broadcast_to(extra[1:2], loss_part.shape)
    col_line = jnp.concatenate([col_lse[i : i + 1] for i in range(TILES)], axis=1)
    row_ids = lax.broadcasted_iota(jnp.int32, (ROWS, BLOCK), 0)
    column_ids = lax.broadcasted_iota(jnp.int32, (ROWS, BLOCK), 1) - pos[2] * ROWS
    own_pairs = jnp.where(row_ids == column_ids, jnp.where(step == 0, 2.0, 0.0), 0.0)
    for k in range(STEP // ROWS):
        span = slice(k * ROWS, (k + 1) * ROWS)
        part = scores[span, :]
        column = as_column(row_lse[pl.ds(step * (STEP // ROWS) + k, 1), :])
        both = jnp.exp(part - column) + jnp.exp(part - col_line)
        if k == 0:
            both = both - own_pairs
        weights[span, :] = both.astype(jnp.bfloat16)
    out = WIRE_SCALE * lax.dot_general(
        weights[...], text[...], NN, preferred_element_type=jnp.float32
    )

    @pl.when(step < HALF // STEP)
    def _():
        near[...] = out

    @pl.when(step >= HALF // STEP)
    def _():
        other[...] = out


def weights_call(pos, scores, row_lse, heard, text):
    half_steps = HALF // STEP
    whole = lambda *shape: pl.BlockSpec(shape, lambda i: (0,) * len(shape))
    rows = pl.BlockSpec((STEP, BLOCK), lambda i: (i, 0))
    width = text.shape[1]
    f32 = jnp.float32
    return pl.pallas_call(
        weights_kernel,
        grid=(BLOCK // STEP,),
        in_specs=[
            pl.BlockSpec(memory_space=pltpu.SMEM),
            rows,
            whole(*row_lse.shape),
            whole(*heard.shape),
            whole(*text.shape),
        ],
        out_specs=[
            rows,
            pl.BlockSpec((STEP, width), lambda i: (jnp.minimum(i, half_steps - 1), 0)),
            pl.BlockSpec((STEP, width), lambda i: (jnp.maximum(i - half_steps, 0), 0)),
            whole(TILES, LANES),
            whole(TILES, LANES),
        ],
        out_shape=[
            jax.ShapeDtypeStruct((BLOCK, BLOCK), jnp.bfloat16),
            jax.ShapeDtypeStruct((HALF, width), f32),
            jax.ShapeDtypeStruct((HALF, width), f32),
            jax.ShapeDtypeStruct((TILES, LANES), f32),
            jax.ShapeDtypeStruct((TILES, LANES), f32),
        ],
        compiler_params=pltpu.CompilerParams(vmem_limit_bytes=VMEM_LIMIT),
        name="weights_kernel",
    )(pos, scores, row_lse, heard, text)


def call(kernel, outs, spec, *args, out_spec=None, scratch=()):
    kinds = {
        "v": pl.BlockSpec(memory_space=pltpu.VMEM),
        "s": pl.BlockSpec(memory_space=pltpu.SMEM),
        "a": pl.BlockSpec(memory_space=pl.ANY),
    }
    return pl.pallas_call(
        kernel,
        out_shape=[jax.ShapeDtypeStruct(*o) for o in outs],
        in_specs=[kinds[k] for k in spec],
        out_specs=[kinds[k] for k in out_spec or "v" * len(outs)],
        scratch_shapes=scratch,
        compiler_params=pltpu.CompilerParams(vmem_limit_bytes=VMEM_LIMIT),
    )(*args)


def parts(image_embed, text_embed, logit_scale):
    f32, f16, bf16 = jnp.float32, jnp.float16, jnp.bfloat16
    width = text_embed.shape[1]
    pos = jnp.stack(
        [lax.axis_index("c"), lax.axis_index("z"), lax.axis_index(PLANE)]
    ).astype(jnp.int32)
    own_image = lax.dynamic_slice_in_dim(image_embed, lax.axis_index("xl") * ROWS, ROWS, 0)

    text_all = exchanged(
        jnp.broadcast_to(text_embed[None], (PLANE_N, ROWS, width)), PLANE
    ).reshape(BLOCK, width)
    near = [own_image] + [None] * (LINE_Z - 1)
    for k, by in ((1, -1), (7, 1), (2, -2), (6, 2), (4, 4)):
        near[k] = shifted(own_image, by)
    near[3] = shifted(near[1], -2)
    near[5] = shifted(near[7], 2)
    far = []
    for block in near:
        far.append(swapped(block))

    message = (PLANE_N, 2 * TILES, LANES)
    scores, image_all, row_message, col_part, diag_part = call(
        scores_kernel,
        [
            ((BLOCK, BLOCK), f32),
            ((BLOCK, width), bf16),
            ((PLANE_N, TILES, LANES), f32),
            ((TILES, LANES), f32),
            ((TILES, LANES), f32),
        ],
        "ss" + "v" * (2 + 2 * LINE_Z),
        pos, logit_scale, text_embed, text_all, *near, *far,
    )
    row_lse, col_message = call(
        rows_kernel,
        [((2 * LINE_Z, LANES), f32), (message, f32)],
        "svvv",
        pos, exchanged(row_message, LINE), col_part, diag_part,
    )
    weights, near_part, other_part, loss_sum, rows_loss = weights_call(
        pos, scores, row_lse, exchanged(col_message, PLANE), text_all
    )
    arrived = swapped(other_part)
    for bit in (1, 2, 4):
        loss_sum = loss_sum + lax.ppermute(
            loss_sum, "z", [(k, k ^ bit) for k in range(LINE_Z)]
        )
    loss_sum = loss_sum + swapped(loss_sum)
    mean_loss = ((rows_loss + loss_sum) * (1.0 / (2 * ROWS * 256)))[0, 0]

    text_part = lax.dot_general(weights, image_all, TN, preferred_element_type=f32)
    text_part = (WIRE_SCALE * text_part).astype(f16).reshape(PLANE_N, ROWS, width)
    text_back = exchanged(text_part, PLANE)
    image_part = [
        near_part[k * ROWS : (k + 1) * ROWS] + arrived[k * ROWS : (k + 1) * ROWS]
        for k in range(LINE_Z)
    ]
    image_sum = image_part[0]
    for k in FAR_FIRST:
        image_sum = image_sum + shifted(image_part[k].astype(f16), k).astype(f32)
    text_sum = text_back[0].astype(f32)
    for k in range(1, PLANE_N):
        text_sum = text_sum + text_back[k].astype(f32)
    factor = logit_scale[0] * (0.5 / WIRE_SCALE)
    return (mean_loss, factor * image_sum, factor * text_sum)


def solution(mesh):
    split = Mesh(mesh.devices.reshape(2, 4, LINE_Z, 2, mesh.shape["rep"]), BATCH_REP)
    return jax.shard_map(
        parts,
        mesh=split,
        in_specs=(P(BATCH, None), P(BATCH_REP, None), P()),
        out_specs=(P(), P(BATCH_REP, None), P(BATCH_REP, None)),
        check_vma=False,
    )
```

```python
import jax
import jax.numpy as jnp
from jax import lax
from jax.experimental import pallas as pl
from jax.experimental.pallas import tpu as pltpu
from jax.sharding import Mesh
from jax.sharding import PartitionSpec as P


BATCH = ("xh", "y", "z", "c")
BATCH_REP = ("xh", "y", "z", "c", "xl")
PLANE = ("xh", "y", "xl")
LINE = ("z", "c")
WIRE_SCALE = 8.0
VMEM_LIMIT = 24 * 1024 * 1024
ROWS = 64
LINE_Z = 8
PLANE_N = 16
HALF = LINE_Z * ROWS
BLOCK = 2 * HALF
LANES = 128
TILES = BLOCK // LANES
STEP = 256
FAR_FIRST = (4, 3, 5, 2, 6, 1, 7)
NT = (((1,), (1,)), ((), ()))
NN = (((1,), (0,)), ((), ()))
TN = (((0,), (0,)), ((), ()))


def exchanged(message, axis):
    return lax.all_to_all(message, axis, 0, 0, tiled=True)


def shifted(array, by):
    return lax.ppermute(array, "z", [(k, (k + by) % LINE_Z) for k in range(LINE_Z)])


def swapped(array):
    return lax.ppermute(array, "c", [(0, 1), (1, 0)])


def as_column(line):
    return jnp.transpose(jnp.broadcast_to(line, (LANES, LANES)))[:ROWS, :1]


def as_line(column):
    return jnp.transpose(jnp.broadcast_to(column, (LANES, LANES)))[:1]


def placed(slots, pos):
    lanes = lax.broadcasted_iota(jnp.int32, (LINE_Z, LANES), 1)
    both = jnp.where(lanes < ROWS, slots[:LINE_Z], pltpu.roll(slots[LINE_Z:], ROWS, 1))
    return pltpu.roll(jnp.where(pos[0] == 0, both, pltpu.roll(both, ROWS, 1)), pos[1], 0)


def relative(both, pos):
    both = pltpu.roll(both, lax.rem(LINE_Z - pos[1], LINE_Z), 0)
    turned = pltpu.roll(both, ROWS, 1)
    same = pos[0] == 0
    return jnp.concatenate(
        [jnp.where(same, both, turned), jnp.where(same, turned, both)], axis=0
    )


def scores_kernel(pos, scale, own_text, text, *refs):
    blocks, rest = refs[: 2 * LINE_Z], refs[2 * LINE_Z :]
    scores, image, row_message, col_part, diag_part = rest
    for k in range(2 * LINE_Z):
        image[k * ROWS : (k + 1) * ROWS, :] = blocks[k][...]
    scale_value = scale[0]
    diag = scale_value * jnp.sum(
        blocks[0][...].astype(jnp.float32) * own_text[...].astype(jnp.float32)
    )
    text_rows = text[...]
    col_max = col_sum = None
    lines = []
    for i in range(BLOCK // STEP):
        span = slice(i * STEP, (i + 1) * STEP)
        part = scale_value * lax.dot_general(
            image[span, :], text_rows, NT, preferred_element_type=jnp.float32
        )
        scores[span, :] = part
        biggest = jnp.max(part, axis=1, keepdims=True)
        lse = biggest + jnp.log(jnp.sum(jnp.exp(part - biggest), axis=1, keepdims=True))
        for t in range(STEP // LANES):
            line = as_line(lse[t * LANES : (t + 1) * LANES])
            lines += [line, pltpu.roll(line, ROWS, 1)]
        top = jnp.max(part, axis=0, keepdims=True)
        new = top if i == 0 else jnp.maximum(col_max, top)
        total = jnp.sum(jnp.exp(part - new), axis=0, keepdims=True)
        col_sum = total if i == 0 else col_sum * jnp.exp(col_max - new) + total
        col_max = new
    message = placed(jnp.concatenate(lines, axis=0), pos)
    diag_part[...] = jnp.full(diag_part.shape, diag)
    row_message[...] = jnp.broadcast_to(message[None], row_message.shape)
    col_lse = col_max + jnp.log(col_sum)
    for i in range(TILES):
        col_part[i : i + 1, :] = col_lse[:, i * LANES : (i + 1) * LANES]


def joined(stats):
    biggest = jnp.max(stats, axis=0)
    return biggest + jnp.log(jnp.sum(jnp.exp(stats - biggest[None]), axis=0))


def rows_kernel(pos, heard, col_part, diag_part, row_lse, col_message):
    lse = joined(heard[...])
    row_lse[...] = relative(lse, pos)
    extra = lax.broadcasted_iota(jnp.int32, (TILES, LANES), 0)
    extra = jnp.where(extra == 0, jnp.sum(lse), diag_part[...])
    message = jnp.concatenate([col_part[...], extra], axis=0)
    col_message[...] = jnp.broadcast_to(message[None], col_message.shape)


def weights_kernel(pos, scores, row_lse, heard, text, weights, near, other, loss_part, rows_loss):
    step = pl.program_id(0)
    col_lse = joined(heard[:, :TILES, :])
    extra = jnp.sum(heard[:, TILES:, :], axis=0)
    rows_loss[...] = jnp.broadcast_to(extra[:1], rows_loss.shape)
    loss_part[...] = jnp.sum(col_lse) - 2.0 * jnp.broadcast_to(extra[1:2], loss_part.shape)
    col_line = jnp.concatenate([col_lse[i : i + 1] for i in range(TILES)], axis=1)
    row_ids = lax.broadcasted_iota(jnp.int32, (ROWS, BLOCK), 0)
    column_ids = lax.broadcasted_iota(jnp.int32, (ROWS, BLOCK), 1) - pos[2] * ROWS
    own_pairs = jnp.where(row_ids == column_ids, jnp.where(step == 0, 2.0, 0.0), 0.0)
    for k in range(STEP // ROWS):
        span = slice(k * ROWS, (k + 1) * ROWS)
        part = scores[span, :]
        column = as_column(row_lse[pl.ds(step * (STEP // ROWS) + k, 1), :])
        both = jnp.exp(part - column) + jnp.exp(part - col_line)
        if k == 0:
            both = both - own_pairs
        weights[span, :] = both.astype(jnp.bfloat16)
    out = WIRE_SCALE * lax.dot_general(
        weights[...], text[...], NN, preferred_element_type=jnp.float32
    )

    @pl.when(step < HALF // STEP)
    def _():
        near[...] = out

    @pl.when(step >= HALF // STEP)
    def _():
        other[...] = out


def weights_call(pos, scores, row_lse, heard, text):
    half_steps = HALF // STEP
    whole = lambda *shape: pl.BlockSpec(shape, lambda i: (0,) * len(shape))
    rows = pl.BlockSpec((STEP, BLOCK), lambda i: (i, 0))
    width = text.shape[1]
    f32 = jnp.float32
    return pl.pallas_call(
        weights_kernel,
        grid=(BLOCK // STEP,),
        in_specs=[
            pl.BlockSpec(memory_space=pltpu.SMEM),
            rows,
            whole(*row_lse.shape),
            whole(*heard.shape),
            whole(*text.shape),
        ],
        out_specs=[
            rows,
            pl.BlockSpec((STEP, width), lambda i: (jnp.minimum(i, half_steps - 1), 0)),
            pl.BlockSpec((STEP, width), lambda i: (jnp.maximum(i - half_steps, 0), 0)),
            whole(TILES, LANES),
            whole(TILES, LANES),
        ],
        out_shape=[
            jax.ShapeDtypeStruct((BLOCK, BLOCK), jnp.bfloat16),
            jax.ShapeDtypeStruct((HALF, width), f32),
            jax.ShapeDtypeStruct((HALF, width), f32),
            jax.ShapeDtypeStruct((TILES, LANES), f32),
            jax.ShapeDtypeStruct((TILES, LANES), f32),
        ],
        compiler_params=pltpu.CompilerParams(vmem_limit_bytes=VMEM_LIMIT),
        name="weights_kernel",
    )(pos, scores, row_lse, heard, text)


def call(kernel, outs, spec, *args, out_spec=None, scratch=()):
    kinds = {
        "v": pl.BlockSpec(memory_space=pltpu.VMEM),
        "s": pl.BlockSpec(memory_space=pltpu.SMEM),
        "a": pl.BlockSpec(memory_space=pl.ANY),
    }
    return pl.pallas_call(
        kernel,
        out_shape=[jax.ShapeDtypeStruct(*o) for o in outs],
        in_specs=[kinds[k] for k in spec],
        out_specs=[kinds[k] for k in out_spec or "v" * len(outs)],
        scratch_shapes=scratch,
        compiler_params=pltpu.CompilerParams(vmem_limit_bytes=VMEM_LIMIT),
    )(*args)


def parts(image_embed, text_embed, logit_scale):
    f32, f16, bf16 = jnp.float32, jnp.float16, jnp.bfloat16
    width = text_embed.shape[1]
    pos = jnp.stack(
        [lax.axis_index("c"), lax.axis_index("z"), lax.axis_index(PLANE)]
    ).astype(jnp.int32)
    own_image = lax.dynamic_slice_in_dim(image_embed, lax.axis_index("xl") * ROWS, ROWS, 0)

    text_all = exchanged(
        jnp.broadcast_to(text_embed[None], (PLANE_N, ROWS, width)), PLANE
    ).reshape(BLOCK, width)
    near = [own_image] + [None] * (LINE_Z - 1)
    for k, by in ((1, -1), (7, 1), (2, -2), (6, 2), (4, 4)):
        near[k] = shifted(own_image, by)
    near[3] = shifted(near[1], -2)
    near[5] = shifted(near[7], 2)
    far = []
    for block in near:
        far.append(swapped(block))

    message = (PLANE_N, 2 * TILES, LANES)
    scores, image_all, row_message, col_part, diag_part = call(
        scores_kernel,
        [
            ((BLOCK, BLOCK), f32),
            ((BLOCK, width), bf16),
            ((PLANE_N, TILES, LANES), f32),
            ((TILES, LANES), f32),
            ((TILES, LANES), f32),
        ],
        "ss" + "v" * (2 + 2 * LINE_Z),
        pos, logit_scale, text_embed, text_all, *near, *far,
    )
    row_lse, col_message = call(
        rows_kernel,
        [((2 * LINE_Z, LANES), f32), (message, f32)],
        "svvv",
        pos, exchanged(row_message, LINE), col_part, diag_part,
    )
    weights, near_part, other_part, loss_sum, rows_loss = weights_call(
        pos, scores, row_lse, exchanged(col_message, PLANE), text_all
    )
    arrived = swapped(other_part)
    loss_sum = loss_sum + swapped(loss_sum)
    for bit in (1, 2, 4):
        loss_sum = loss_sum + lax.ppermute(
            loss_sum, "z", [(k, k ^ bit) for k in range(LINE_Z)]
        )
    mean_loss = ((rows_loss + loss_sum) * (1.0 / (2 * ROWS * 256)))[0, 0]

    text_part = lax.dot_general(weights, image_all, TN, preferred_element_type=f32)
    text_part = (WIRE_SCALE * text_part).astype(f16).reshape(PLANE_N, ROWS, width)
    text_back = exchanged(text_part, PLANE)
    factor = logit_scale[0] * (0.5 / WIRE_SCALE)
    image_part = [
        near_part[k * ROWS : (k + 1) * ROWS] + arrived[k * ROWS : (k + 1) * ROWS]
        for k in range(LINE_Z)
    ]
    leaving = [part.astype(f16) for part in image_part]
    back = {}
    for k in FAR_FIRST:
        back[k] = shifted(leaving[k], k)
    text_sum = text_back[0].astype(f32)
    for k in range(1, PLANE_N):
        text_sum = text_sum + text_back[k].astype(f32)
    text_grad = factor * text_sum
    image_sum = image_part[0]
    for k in FAR_FIRST[:5]:
        image_sum = image_sum + back[k].astype(f32)
    image_sum = lax.optimization_barrier(image_sum)
    for k in FAR_FIRST[5:]:
        image_sum = image_sum + back[k].astype(f32)
    image_grad = factor * image_sum
    return (mean_loss, image_grad, text_grad)


def solution(mesh):
    split = Mesh(mesh.devices.reshape(2, 4, LINE_Z, 2, mesh.shape["rep"]), BATCH_REP)
    return jax.shard_map(
        parts,
        mesh=split,
        in_specs=(P(BATCH, None), P(BATCH_REP, None), P()),
        out_specs=(P(), P(BATCH_REP, None), P(BATCH_REP, None)),
        check_vma=False,
    )
```

```python
import jax
import jax.numpy as jnp
from jax import lax
from jax.experimental import pallas as pl
from jax.experimental.pallas import tpu as pltpu
from jax.sharding import Mesh
from jax.sharding import PartitionSpec as P


BATCH = ("xh", "y", "z", "c")
BATCH_REP = ("xh", "y", "z", "c", "xl")
PLANE = ("xh", "y", "xl")
LINE = ("z", "c")
WIRE_SCALE = 8.0
VMEM_LIMIT = 24 * 1024 * 1024
ROWS = 64
LINE_Z = 8
PLANE_N = 16
HALF = LINE_Z * ROWS
BLOCK = 2 * HALF
LANES = 128
TILES = BLOCK // LANES
STEP = 256
FAR_FIRST = (4, 3, 5, 2, 6, 1, 7)
NT = (((1,), (1,)), ((), ()))
NN = (((1,), (0,)), ((), ()))
TN = (((0,), (0,)), ((), ()))


def exchanged(message, axis):
    return lax.all_to_all(message, axis, 0, 0, tiled=True)


def shifted(array, by):
    return lax.ppermute(array, "z", [(k, (k + by) % LINE_Z) for k in range(LINE_Z)])


def across(array, bit):
    return lax.ppermute(array, "z", [(k, k ^ bit) for k in range(LINE_Z)])


def swapped(array):
    return lax.ppermute(array, "c", [(0, 1), (1, 0)])


def as_column(line):
    return jnp.transpose(jnp.broadcast_to(line, (LANES, LANES)))[:ROWS, :1]


def as_line(column):
    return jnp.transpose(jnp.broadcast_to(column, (LANES, LANES)))[:1]


def placed(slots, pos):
    lanes = lax.broadcasted_iota(jnp.int32, (LINE_Z, LANES), 1)
    both = jnp.where(lanes < ROWS, slots[:LINE_Z], pltpu.roll(slots[LINE_Z:], ROWS, 1))
    return pltpu.roll(jnp.where(pos[0] == 0, both, pltpu.roll(both, ROWS, 1)), pos[1], 0)


def relative(both, pos):
    both = pltpu.roll(both, lax.rem(LINE_Z - pos[1], LINE_Z), 0)
    turned = pltpu.roll(both, ROWS, 1)
    same = pos[0] == 0
    return jnp.concatenate(
        [jnp.where(same, both, turned), jnp.where(same, turned, both)], axis=0
    )


def scores_kernel(pos, scale, own_text, text, *refs):
    blocks, rest = refs[: 2 * LINE_Z], refs[2 * LINE_Z :]
    scores, image, row_message, col_part, diag_part = rest
    for k in range(2 * LINE_Z):
        image[k * ROWS : (k + 1) * ROWS, :] = blocks[k][...]
    scale_value = scale[0]
    diag = scale_value * jnp.sum(
        blocks[0][...].astype(jnp.float32) * own_text[...].astype(jnp.float32)
    )
    text_rows = text[...]
    col_max = col_sum = None
    lines = []
    for i in range(BLOCK // STEP):
        span = slice(i * STEP, (i + 1) * STEP)
        part = scale_value * lax.dot_general(
            image[span, :], text_rows, NT, preferred_element_type=jnp.float32
        )
        scores[span, :] = part
        biggest = jnp.max(part, axis=1, keepdims=True)
        lse = biggest + jnp.log(jnp.sum(jnp.exp(part - biggest), axis=1, keepdims=True))
        for t in range(STEP // LANES):
            line = as_line(lse[t * LANES : (t + 1) * LANES])
            lines += [line, pltpu.roll(line, ROWS, 1)]
        top = jnp.max(part, axis=0, keepdims=True)
        new = top if i == 0 else jnp.maximum(col_max, top)
        total = jnp.sum(jnp.exp(part - new), axis=0, keepdims=True)
        col_sum = total if i == 0 else col_sum * jnp.exp(col_max - new) + total
        col_max = new
    message = placed(jnp.concatenate(lines, axis=0), pos)
    diag_part[...] = jnp.full(diag_part.shape, diag)
    row_message[...] = jnp.broadcast_to(message[None], row_message.shape)
    col_lse = col_max + jnp.log(col_sum)
    for i in range(TILES):
        col_part[i : i + 1, :] = col_lse[:, i * LANES : (i + 1) * LANES]


def joined(stats):
    biggest = jnp.max(stats, axis=0)
    return biggest + jnp.log(jnp.sum(jnp.exp(stats - biggest[None]), axis=0))


def rows_kernel(pos, heard, col_part, diag_part, row_lse, col_message):
    lse = joined(heard[...])
    row_lse[...] = relative(lse, pos)
    extra = lax.broadcasted_iota(jnp.int32, (TILES, LANES), 0)
    extra = jnp.where(extra == 0, jnp.sum(lse), diag_part[...])
    message = jnp.concatenate([col_part[...], extra], axis=0)
    col_message[...] = jnp.broadcast_to(message[None], col_message.shape)


def weights_kernel(
    pos, scores, row_lse, heard, text, weights, near, other_out, loss_part, rows_loss, other, sems
):
    col_lse = joined(heard[:, :TILES, :])
    extra = jnp.sum(heard[:, TILES:, :], axis=0)
    rows_loss[...] = jnp.broadcast_to(extra[:1], rows_loss.shape)
    loss_part[...] = jnp.sum(col_lse) - 2.0 * jnp.broadcast_to(extra[1:2], loss_part.shape)
    col_line = jnp.concatenate([col_lse[i : i + 1] for i in range(TILES)], axis=1)
    text_rows = text[...]
    copies = []
    half_steps = HALF // STEP
    for step in [*range(half_steps, 2 * half_steps), *range(half_steps)]:
        blocks = []
        for k in range(STEP // ROWS * step, STEP // ROWS * (step + 1)):
            part = scores[k * ROWS : (k + 1) * ROWS, :]
            both = jnp.exp(part - as_column(row_lse[k : k + 1, :])) + jnp.exp(part - col_line)
            if k == 0:
                row_ids = lax.broadcasted_iota(jnp.int32, part.shape, 0)
                column_ids = lax.broadcasted_iota(jnp.int32, part.shape, 1) - pos[2] * ROWS
                both = both - 2.0 * (row_ids == column_ids).astype(jnp.float32)
            blocks.append(both.astype(jnp.bfloat16))
        rows = jnp.concatenate(blocks, axis=0)
        weights[step * STEP : (step + 1) * STEP, :] = rows
        out = WIRE_SCALE * lax.dot_general(rows, text_rows, NN, preferred_element_type=jnp.float32)
        span = slice(step % half_steps * STEP, (step % half_steps + 1) * STEP)
        if step < half_steps:
            near[span, :] = out
        else:
            other[span, :] = out
            copies.append(
                pltpu.make_async_copy(other.at[span, :], other_out.at[span, :], sems.at[len(copies)])
            )
            copies[-1].start()
    for copy in copies:
        copy.wait()


def call(kernel, outs, spec, *args, out_spec=None, scratch=()):
    kinds = {
        "v": pl.BlockSpec(memory_space=pltpu.VMEM),
        "s": pl.BlockSpec(memory_space=pltpu.SMEM),
        "a": pl.BlockSpec(memory_space=pl.ANY),
    }
    return pl.pallas_call(
        kernel,
        out_shape=[jax.ShapeDtypeStruct(*o) for o in outs],
        in_specs=[kinds[k] for k in spec],
        out_specs=[kinds[k] for k in out_spec or "v" * len(outs)],
        scratch_shapes=scratch,
        compiler_params=pltpu.CompilerParams(vmem_limit_bytes=VMEM_LIMIT),
    )(*args)


def parts(image_embed, text_embed, logit_scale):
    f32, f16, bf16 = jnp.float32, jnp.float16, jnp.bfloat16
    width = text_embed.shape[1]
    pos = jnp.stack(
        [lax.axis_index("c"), lax.axis_index("z"), lax.axis_index(PLANE)]
    ).astype(jnp.int32)
    own_image = lax.dynamic_slice_in_dim(image_embed, lax.axis_index("xl") * ROWS, ROWS, 0)

    text_all = exchanged(
        jnp.broadcast_to(text_embed[None], (PLANE_N, ROWS, width)), PLANE
    ).reshape(BLOCK, width)
    near = [own_image] + [None] * (LINE_Z - 1)
    for k, by in ((1, -1), (7, 1), (2, -2), (6, 2), (4, 4)):
        near[k] = shifted(own_image, by)
    near[3] = shifted(near[1], -2)
    near[5] = shifted(near[7], 2)
    far = []
    for block in near:
        far.append(swapped(block))

    message = (PLANE_N, 2 * TILES, LANES)
    scores, image_all, row_message, col_part, diag_part = call(
        scores_kernel,
        [
            ((BLOCK, BLOCK), f32),
            ((BLOCK, width), bf16),
            ((PLANE_N, TILES, LANES), f32),
            ((TILES, LANES), f32),
            ((TILES, LANES), f32),
        ],
        "ss" + "v" * (2 + 2 * LINE_Z),
        pos, logit_scale, text_embed, text_all, *near, *far,
    )
    row_lse, col_message = call(
        rows_kernel,
        [((2 * LINE_Z, LANES), f32), (message, f32)],
        "svvv",
        pos, exchanged(row_message, LINE), col_part, diag_part,
    )
    weights, near_part, other_part, loss_sum, rows_loss = call(
        weights_kernel,
        [
            ((BLOCK, BLOCK), bf16),
            ((HALF, width), f32),
            ((HALF, width), f32),
            ((TILES, LANES), f32),
            ((TILES, LANES), f32),
        ],
        "svvvv",
        pos, scores, row_lse, exchanged(col_message, PLANE), text_all,
        out_spec="vvavv",
        scratch=[pltpu.VMEM((HALF, width), f32), pltpu.SemaphoreType.DMA((HALF // STEP,))],
    )
    arrived = swapped(other_part)
    loss_sum = loss_sum + swapped(loss_sum)
    for bit in (1, 2):
        loss_sum = loss_sum + across(loss_sum, bit)
    crossed = across(loss_sum, 4)
    mean_loss = ((rows_loss + (loss_sum + crossed)) * (1.0 / (2 * ROWS * 256)))[0, 0]

    text_part = lax.dot_general(weights, image_all, TN, preferred_element_type=f32)
    text_part = (WIRE_SCALE * text_part).astype(f16).reshape(PLANE_N, ROWS, width)
    text_back = exchanged(text_part, PLANE)
    factor = logit_scale[0] * (0.5 / WIRE_SCALE)
    image_part = [
        near_part[k * ROWS : (k + 1) * ROWS] + arrived[k * ROWS : (k + 1) * ROWS]
        for k in range(LINE_Z)
    ]
    leaving = [part.astype(f16) for part in image_part]
    back = {}
    for k in FAR_FIRST:
        back[k] = shifted(leaving[k], k)
    text_sum = text_back[0].astype(f32)
    for k in range(1, PLANE_N):
        text_sum = text_sum + text_back[k].astype(f32)
    text_grad = factor * text_sum
    image_sum = image_part[0]
    for k in FAR_FIRST[:5]:
        image_sum = image_sum + back[k].astype(f32)
    image_sum = lax.optimization_barrier(image_sum)
    for k in FAR_FIRST[5:]:
        image_sum = image_sum + back[k].astype(f32)
    image_grad = factor * image_sum
    return (mean_loss, image_grad, text_grad)


def solution(mesh):
    split = Mesh(mesh.devices.reshape(2, 4, LINE_Z, 2, mesh.shape["rep"]), BATCH_REP)
    return jax.shard_map(
        parts,
        mesh=split,
        in_specs=(P(BATCH, None), P(BATCH_REP, None), P()),
        out_specs=(P(), P(BATCH_REP, None), P(BATCH_REP, None)),
        check_vma=False,
    )
```

```python
import jax
import jax.numpy as jnp
from jax import lax
from jax.experimental import pallas as pl
from jax.experimental.pallas import tpu as pltpu
from jax.sharding import Mesh
from jax.sharding import PartitionSpec as P


BATCH = ("xh", "y", "z", "c")
BATCH_REP = ("xh", "y", "z", "c", "xl")
PLANE = ("xh", "y", "xl")
LINE = ("z", "c")
WIRE_SCALE = 8.0
VMEM_LIMIT = 24 * 1024 * 1024
ROWS = 64
LINE_Z = 8
PLANE_N = 16
HALF = LINE_Z * ROWS
BLOCK = 2 * HALF
LANES = 128
TILES = BLOCK // LANES
STEP = 256
FAR_FIRST = (4, 3, 5, 2, 6, 1, 7)
NT = (((1,), (1,)), ((), ()))
NN = (((1,), (0,)), ((), ()))
TN = (((0,), (0,)), ((), ()))


def exchanged(message, axis):
    return lax.all_to_all(message, axis, 0, 0, tiled=True)


def shifted(array, by):
    return lax.ppermute(array, "z", [(k, (k + by) % LINE_Z) for k in range(LINE_Z)])


def across(array, bit):
    return lax.ppermute(array, "z", [(k, k ^ bit) for k in range(LINE_Z)])


def swapped(array):
    return lax.ppermute(array, "c", [(0, 1), (1, 0)])


def as_column(line):
    return jnp.transpose(jnp.broadcast_to(line, (LANES, LANES)))[:ROWS, :1]


def as_line(column):
    return jnp.transpose(jnp.broadcast_to(column, (LANES, LANES)))[:1]


def placed(slots, pos):
    lanes = lax.broadcasted_iota(jnp.int32, (LINE_Z, LANES), 1)
    both = jnp.where(lanes < ROWS, slots[:LINE_Z], pltpu.roll(slots[LINE_Z:], ROWS, 1))
    return pltpu.roll(jnp.where(pos[0] == 0, both, pltpu.roll(both, ROWS, 1)), pos[1], 0)


def relative(both, pos):
    both = pltpu.roll(both, lax.rem(LINE_Z - pos[1], LINE_Z), 0)
    turned = pltpu.roll(both, ROWS, 1)
    same = pos[0] == 0
    return jnp.concatenate(
        [jnp.where(same, both, turned), jnp.where(same, turned, both)], axis=0
    )


def scores_kernel(pos, scale, own_text, text, *refs):
    blocks, rest = refs[: 2 * LINE_Z], refs[2 * LINE_Z :]
    scores, image, row_message, col_part, diag_part = rest
    for k in range(2 * LINE_Z):
        image[k * ROWS : (k + 1) * ROWS, :] = blocks[k][...]
    scale_value = scale[0]
    diag = scale_value * jnp.sum(
        blocks[0][...].astype(jnp.float32) * own_text[...].astype(jnp.float32)
    )
    text_rows = text[...]
    col_max = col_sum = None
    lines = []
    for i in range(BLOCK // STEP):
        span = slice(i * STEP, (i + 1) * STEP)
        part = scale_value * lax.dot_general(
            image[span, :], text_rows, NT, preferred_element_type=jnp.float32
        )
        scores[span, :] = part
        biggest = jnp.max(part, axis=1, keepdims=True)
        lse = biggest + jnp.log(jnp.sum(jnp.exp(part - biggest), axis=1, keepdims=True))
        for t in range(STEP // LANES):
            line = as_line(lse[t * LANES : (t + 1) * LANES])
            lines += [line, pltpu.roll(line, ROWS, 1)]
        top = jnp.max(part, axis=0, keepdims=True)
        new = top if i == 0 else jnp.maximum(col_max, top)
        total = jnp.sum(jnp.exp(part - new), axis=0, keepdims=True)
        col_sum = total if i == 0 else col_sum * jnp.exp(col_max - new) + total
        col_max = new
    message = placed(jnp.concatenate(lines, axis=0), pos)
    diag_part[...] = jnp.full(diag_part.shape, diag)
    row_message[...] = jnp.broadcast_to(message[None], row_message.shape)
    col_lse = col_max + jnp.log(col_sum)
    for i in range(TILES):
        col_part[i : i + 1, :] = col_lse[:, i * LANES : (i + 1) * LANES]


def joined(stats):
    biggest = jnp.max(stats, axis=0)
    return biggest + jnp.log(jnp.sum(jnp.exp(stats - biggest[None]), axis=0))


def rows_kernel(pos, heard, col_part, diag_part, row_lse, col_message):
    lse = joined(heard[...])
    row_lse[...] = relative(lse, pos)
    extra = lax.broadcasted_iota(jnp.int32, (TILES, LANES), 0)
    extra = jnp.where(extra == 0, jnp.sum(lse), diag_part[...])
    message = jnp.concatenate([col_part[...], extra], axis=0)
    col_message[...] = jnp.broadcast_to(message[None], col_message.shape)


def weights_kernel(
    pos, scores, row_lse, heard, text, weights, near, other_out, loss_part, rows_loss, other, sems
):
    col_lse = joined(heard[:, :TILES, :])
    extra = jnp.sum(heard[:, TILES:, :], axis=0)
    rows_loss[...] = jnp.broadcast_to(extra[:1], rows_loss.shape)
    loss_part[...] = jnp.sum(col_lse) - 2.0 * jnp.broadcast_to(extra[1:2], loss_part.shape)
    col_line = jnp.concatenate([col_lse[i : i + 1] for i in range(TILES)], axis=1)
    text_rows = text[...]
    copies = []
    half_steps = HALF // STEP
    for step in [*range(half_steps, 2 * half_steps), *range(half_steps)]:
        blocks = []
        for k in range(STEP // ROWS * step, STEP // ROWS * (step + 1)):
            part = scores[k * ROWS : (k + 1) * ROWS, :]
            both = jnp.exp(part - as_column(row_lse[k : k + 1, :])) + jnp.exp(part - col_line)
            if k == 0:
                row_ids = lax.broadcasted_iota(jnp.int32, part.shape, 0)
                column_ids = lax.broadcasted_iota(jnp.int32, part.shape, 1) - pos[2] * ROWS
                both = both - 2.0 * (row_ids == column_ids).astype(jnp.float32)
            blocks.append(both.astype(jnp.bfloat16))
        rows = jnp.concatenate(blocks, axis=0)
        weights[step * STEP : (step + 1) * STEP, :] = rows
        out = WIRE_SCALE * lax.dot_general(rows, text_rows, NN, preferred_element_type=jnp.float32)
        span = slice(step % half_steps * STEP, (step % half_steps + 1) * STEP)
        if step < half_steps:
            near[span, :] = out
        else:
            other[span, :] = out
            copies.append(
                pltpu.make_async_copy(other.at[span, :], other_out.at[span, :], sems.at[len(copies)])
            )
            copies[-1].start()
    for copy in copies:
        copy.wait()


def call(kernel, outs, spec, *args, out_spec=None, scratch=()):
    kinds = {
        "v": pl.BlockSpec(memory_space=pltpu.VMEM),
        "s": pl.BlockSpec(memory_space=pltpu.SMEM),
        "a": pl.BlockSpec(memory_space=pl.ANY),
    }
    return pl.pallas_call(
        kernel,
        out_shape=[jax.ShapeDtypeStruct(*o) for o in outs],
        in_specs=[kinds[k] for k in spec],
        out_specs=[kinds[k] for k in out_spec or "v" * len(outs)],
        scratch_shapes=scratch,
        compiler_params=pltpu.CompilerParams(vmem_limit_bytes=VMEM_LIMIT),
    )(*args)


def parts(image_embed, text_embed, logit_scale):
    f32, f16, bf16 = jnp.float32, jnp.float16, jnp.bfloat16
    width = text_embed.shape[1]
    pos = jnp.stack(
        [lax.axis_index("c"), lax.axis_index("z"), lax.axis_index(PLANE)]
    ).astype(jnp.int32)
    own_image = lax.dynamic_slice_in_dim(image_embed, lax.axis_index("xl") * ROWS, ROWS, 0)

    text_all = exchanged(
        jnp.broadcast_to(text_embed[None], (PLANE_N, ROWS, width)), PLANE
    ).reshape(BLOCK, width)
    near = [own_image] + [None] * (LINE_Z - 1)
    for k, by in ((1, -1), (7, 1), (2, -2), (6, 2), (4, 4)):
        near[k] = shifted(own_image, by)
    near[3] = shifted(near[1], -2)
    near[5] = shifted(near[7], 2)
    far = []
    for k, block in enumerate(near):
        far.append(swapped(block))

    message = (PLANE_N, 2 * TILES, LANES)
    scores, image_all, row_message, col_part, diag_part = call(
        scores_kernel,
        [
            ((BLOCK, BLOCK), f32),
            ((BLOCK, width), bf16),
            ((PLANE_N, TILES, LANES), f32),
            ((TILES, LANES), f32),
            ((TILES, LANES), f32),
        ],
        "ss" + "v" * (2 + 2 * LINE_Z),
        pos, logit_scale, text_embed, text_all, *near, *far,
    )
    row_lse, col_message = call(
        rows_kernel,
        [((2 * LINE_Z, LANES), f32), (message, f32)],
        "svvv",
        pos, exchanged(row_message, LINE), col_part, diag_part,
    )
    weights, near_part, other_part, loss_sum, rows_loss = call(
        weights_kernel,
        [
            ((BLOCK, BLOCK), bf16),
            ((HALF, width), f32),
            ((HALF, width), f32),
            ((TILES, LANES), f32),
            ((TILES, LANES), f32),
        ],
        "svvvv",
        pos, scores, row_lse, exchanged(col_message, PLANE), text_all,
        out_spec="vvavv",
        scratch=[pltpu.VMEM((HALF, width), f32), pltpu.SemaphoreType.DMA((HALF // STEP,))],
    )
    arrived = swapped(other_part)
    loss_sum = loss_sum + swapped(loss_sum)
    loss_sum = loss_sum + across(loss_sum, 1)
    apart = {}
    for bits in (4, 2, 6):
        apart[bits] = across(loss_sum, bits)
    loss_sum = (loss_sum + apart[4]) + (apart[2] + apart[6])
    mean_loss = ((rows_loss + loss_sum) * (1.0 / (2 * ROWS * 256)))[0, 0]

    text_part = lax.dot_general(weights, image_all, TN, preferred_element_type=f32)
    text_part = (WIRE_SCALE * text_part).astype(f16).reshape(PLANE_N, ROWS, width)
    text_back = exchanged(text_part, PLANE)
    factor = logit_scale[0] * (0.5 / WIRE_SCALE)
    leaving = {}
    near_rest, arrived_rest = lax.optimization_barrier((near_part, arrived))
    for parts_of, blocks in (
        ((near_part, arrived), FAR_FIRST[:3]), ((near_rest, arrived_rest), FAR_FIRST[3:])
    ):
        for k in blocks:
            here, there = (part[k * ROWS : (k + 1) * ROWS] for part in parts_of)
            leaving[k] = (here + there).astype(f16)
    back = {}
    for k in FAR_FIRST:
        back[k] = shifted(leaving[k], k)
    text_sum = text_back[0].astype(f32)
    for k in range(1, PLANE_N):
        text_sum = text_sum + text_back[k].astype(f32)
    text_grad = factor * text_sum
    image_sum = near_part[:ROWS] + arrived[:ROWS]
    for k in FAR_FIRST[:3]:
        image_sum = image_sum + back[k].astype(f32)
    image_sum = lax.optimization_barrier(image_sum)
    for k in FAR_FIRST[3:]:
        image_sum = image_sum + back[k].astype(f32)
    image_grad = factor * image_sum
    return (mean_loss, image_grad, text_grad)


def solution(mesh):
    split = Mesh(mesh.devices.reshape(2, 4, LINE_Z, 2, mesh.shape["rep"]), BATCH_REP)
    return jax.shard_map(
        parts,
        mesh=split,
        in_specs=(P(BATCH, None), P(BATCH_REP, None), P()),
        out_specs=(P(), P(BATCH_REP, None), P(BATCH_REP, None)),
        check_vma=False,
    )
```

```python
import jax
import jax.numpy as jnp
from jax import lax
from jax.experimental import pallas as pl
from jax.experimental.pallas import tpu as pltpu
from jax.sharding import Mesh
from jax.sharding import PartitionSpec as P


BATCH = ("xh", "y", "z", "c")
BATCH_REP = ("xh", "y", "z", "c", "xl")
PLANE = ("xh", "y", "xl")
LINE = ("z", "c")
WIRE_SCALE = 8.0
VMEM_LIMIT = 24 * 1024 * 1024
ROWS = 64
LINE_Z = 8
PLANE_N = 16
HALF = LINE_Z * ROWS
BLOCK = 2 * HALF
LANES = 128
TILES = BLOCK // LANES
STEP = 256
FAR_FIRST = (4, 3, 5, 2, 6, 1, 7)
NT = (((1,), (1,)), ((), ()))
NN = (((1,), (0,)), ((), ()))
TN = (((0,), (0,)), ((), ()))


def exchanged(message, axis):
    return lax.all_to_all(message, axis, 0, 0, tiled=True)


def shifted(array, by):
    return lax.ppermute(array, "z", [(k, (k + by) % LINE_Z) for k in range(LINE_Z)])


def across(array, bit):
    return lax.ppermute(array, "z", [(k, k ^ bit) for k in range(LINE_Z)])


def swapped(array):
    return lax.ppermute(array, "c", [(0, 1), (1, 0)])


def as_column(line):
    return jnp.transpose(jnp.broadcast_to(line, (LANES, LANES)))[:ROWS, :1]


def as_line(column):
    return jnp.transpose(jnp.broadcast_to(column, (LANES, LANES)))[:1]


def placed(slots, pos):
    lanes = lax.broadcasted_iota(jnp.int32, (LINE_Z, LANES), 1)
    both = jnp.where(lanes < ROWS, slots[:LINE_Z], pltpu.roll(slots[LINE_Z:], ROWS, 1))
    return pltpu.roll(jnp.where(pos[0] == 0, both, pltpu.roll(both, ROWS, 1)), pos[1], 0)


def relative(both, pos):
    both = pltpu.roll(both, lax.rem(LINE_Z - pos[1], LINE_Z), 0)
    turned = pltpu.roll(both, ROWS, 1)
    same = pos[0] == 0
    return jnp.concatenate(
        [jnp.where(same, both, turned), jnp.where(same, turned, both)], axis=0
    )


def scores_kernel(pos, scale, own_text, text, *refs):
    blocks, rest = refs[: 2 * LINE_Z], refs[2 * LINE_Z :]
    scores, image, row_message, col_part, diag_part = rest
    for k in range(2 * LINE_Z):
        image[k * ROWS : (k + 1) * ROWS, :] = blocks[k][...]
    scale_value = scale[0]
    diag = scale_value * jnp.sum(
        blocks[0][...].astype(jnp.float32) * own_text[...].astype(jnp.float32)
    )
    text_rows = text[...]
    col_max = col_sum = None
    lines = []
    for i in range(BLOCK // STEP):
        span = slice(i * STEP, (i + 1) * STEP)
        part = scale_value * lax.dot_general(
            image[span, :], text_rows, NT, preferred_element_type=jnp.float32
        )
        scores[span, :] = part
        biggest = jnp.max(part, axis=1, keepdims=True)
        lse = biggest + jnp.log(jnp.sum(jnp.exp(part - biggest), axis=1, keepdims=True))
        for t in range(STEP // LANES):
            line = as_line(lse[t * LANES : (t + 1) * LANES])
            lines += [line, pltpu.roll(line, ROWS, 1)]
        top = jnp.max(part, axis=0, keepdims=True)
        new = top if i == 0 else jnp.maximum(col_max, top)
        total = jnp.sum(jnp.exp(part - new), axis=0, keepdims=True)
        col_sum = total if i == 0 else col_sum * jnp.exp(col_max - new) + total
        col_max = new
    message = placed(jnp.concatenate(lines, axis=0), pos)
    diag_part[...] = jnp.full(diag_part.shape, diag)
    row_message[...] = jnp.broadcast_to(message[None], row_message.shape)
    col_lse = col_max + jnp.log(col_sum)
    for i in range(TILES):
        col_part[i : i + 1, :] = col_lse[:, i * LANES : (i + 1) * LANES]


def joined(stats):
    biggest = jnp.max(stats, axis=0)
    return biggest + jnp.log(jnp.sum(jnp.exp(stats - biggest[None]), axis=0))


def rows_kernel(pos, heard, col_part, diag_part, row_lse, col_message):
    lse = joined(heard[...])
    row_lse[...] = relative(lse, pos)
    extra = lax.broadcasted_iota(jnp.int32, (TILES, LANES), 0)
    extra = jnp.where(extra == 0, jnp.sum(lse), diag_part[...])
    message = jnp.concatenate([col_part[...], extra], axis=0)
    col_message[...] = jnp.broadcast_to(message[None], col_message.shape)


def weights_kernel(
    pos, scores, row_lse, heard, text, weights, near, other_out, loss_part, rows_loss, other, sems
):
    col_lse = joined(heard[:, :TILES, :])
    extra = jnp.sum(heard[:, TILES:, :], axis=0)
    rows_loss[...] = jnp.broadcast_to(extra[:1], rows_loss.shape)
    loss_part[...] = jnp.sum(col_lse) - 2.0 * jnp.broadcast_to(extra[1:2], loss_part.shape)
    col_line = jnp.concatenate([col_lse[i : i + 1] for i in range(TILES)], axis=1)
    text_rows = text[...]
    copies = []
    half_steps = HALF // STEP
    for step in [*range(half_steps, 2 * half_steps), *range(half_steps)]:
        blocks = []
        for k in range(STEP // ROWS * step, STEP // ROWS * (step + 1)):
            part = scores[k * ROWS : (k + 1) * ROWS, :]
            both = jnp.exp(part - as_column(row_lse[k : k + 1, :])) + jnp.exp(part - col_line)
            if k == 0:
                row_ids = lax.broadcasted_iota(jnp.int32, part.shape, 0)
                column_ids = lax.broadcasted_iota(jnp.int32, part.shape, 1) - pos[2] * ROWS
                both = both - 2.0 * (row_ids == column_ids).astype(jnp.float32)
            blocks.append(both.astype(jnp.bfloat16))
        rows = jnp.concatenate(blocks, axis=0)
        weights[step * STEP : (step + 1) * STEP, :] = rows
        out = WIRE_SCALE * lax.dot_general(rows, text_rows, NN, preferred_element_type=jnp.float32)
        span = slice(step % half_steps * STEP, (step % half_steps + 1) * STEP)
        if step < half_steps:
            near[span, :] = out
        else:
            other[span, :] = out
            copies.append(
                pltpu.make_async_copy(other.at[span, :], other_out.at[span, :], sems.at[len(copies)])
            )
            copies[-1].start()
    for copy in copies:
        copy.wait()


def call(kernel, outs, spec, *args, out_spec=None, scratch=()):
    kinds = {
        "v": pl.BlockSpec(memory_space=pltpu.VMEM),
        "s": pl.BlockSpec(memory_space=pltpu.SMEM),
        "a": pl.BlockSpec(memory_space=pl.ANY),
    }
    return pl.pallas_call(
        kernel,
        out_shape=[jax.ShapeDtypeStruct(*o) for o in outs],
        in_specs=[kinds[k] for k in spec],
        out_specs=[kinds[k] for k in out_spec or "v" * len(outs)],
        scratch_shapes=scratch,
        compiler_params=pltpu.CompilerParams(vmem_limit_bytes=VMEM_LIMIT),
    )(*args)


def parts(image_embed, text_embed, logit_scale):
    f32, f16, bf16 = jnp.float32, jnp.float16, jnp.bfloat16
    width = text_embed.shape[1]
    pos = jnp.stack(
        [lax.axis_index("c"), lax.axis_index("z"), lax.axis_index(PLANE)]
    ).astype(jnp.int32)
    own_image = lax.dynamic_slice_in_dim(image_embed, lax.axis_index("xl") * ROWS, ROWS, 0)

    text_all = exchanged(
        jnp.broadcast_to(text_embed[None], (PLANE_N, ROWS, width)), PLANE
    ).reshape(BLOCK, width)
    near = [own_image] + [None] * (LINE_Z - 1)
    for k, by in ((1, -1), (7, 1), (2, -2), (6, 2), (4, 4)):
        near[k] = shifted(own_image, by)
    near[3] = shifted(near[1], -2)
    near[5] = shifted(near[7], 2)
    far = []
    for block in near:
        far.append(swapped(block))

    message = (PLANE_N, 2 * TILES, LANES)
    scores, image_all, row_message, col_part, diag_part = call(
        scores_kernel,
        [
            ((BLOCK, BLOCK), f32),
            ((BLOCK, width), bf16),
            ((PLANE_N, TILES, LANES), f32),
            ((TILES, LANES), f32),
            ((TILES, LANES), f32),
        ],
        "ss" + "v" * (2 + 2 * LINE_Z),
        pos, logit_scale, text_embed, text_all, *near, *far,
    )
    row_lse, col_message = call(
        rows_kernel,
        [((2 * LINE_Z, LANES), f32), (message, f32)],
        "svvv",
        pos, exchanged(row_message, LINE), col_part, diag_part,
    )
    weights, near_part, other_part, loss_sum, rows_loss = call(
        weights_kernel,
        [
            ((BLOCK, BLOCK), bf16),
            ((HALF, width), f32),
            ((HALF, width), f32),
            ((TILES, LANES), f32),
            ((TILES, LANES), f32),
        ],
        "svvvv",
        pos, scores, row_lse, exchanged(col_message, PLANE), text_all,
        out_spec="vvavv",
        scratch=[pltpu.VMEM((HALF, width), f32), pltpu.SemaphoreType.DMA((HALF // STEP,))],
    )
    arrived = swapped(other_part)
    loss_sum = loss_sum + swapped(loss_sum)
    loss_sum = loss_sum + across(loss_sum, 1)
    apart = {}
    for bits in (4, 2, 6):
        apart[bits] = across(loss_sum, bits)
    loss_sum = (loss_sum + apart[4]) + (apart[2] + apart[6])
    mean_loss = ((rows_loss + loss_sum) * (1.0 / (2 * ROWS * 256)))[0, 0]

    text_part = lax.dot_general(weights, image_all, TN, preferred_element_type=f32)
    text_part = (WIRE_SCALE * text_part).astype(f16).reshape(PLANE_N, ROWS, width)
    text_back = exchanged(text_part, PLANE)
    factor = logit_scale[0] * (0.5 / WIRE_SCALE)
    image_part = [
        near_part[k * ROWS : (k + 1) * ROWS] + arrived[k * ROWS : (k + 1) * ROWS]
        for k in range(LINE_Z)
    ]
    leaving = [part.astype(f16) for part in image_part]
    back = {}
    for k in FAR_FIRST:
        back[k] = shifted(leaving[k], k)
    text_sum = text_back[0].astype(f32)
    for k in range(1, PLANE_N):
        text_sum = text_sum + text_back[k].astype(f32)
    text_grad = factor * text_sum
    image_sum = image_part[0]
    for k in FAR_FIRST[:5]:
        image_sum = image_sum + back[k].astype(f32)
    image_sum = lax.optimization_barrier(image_sum)
    for k in FAR_FIRST[5:]:
        image_sum = image_sum + back[k].astype(f32)
    image_grad = factor * image_sum
    return (mean_loss, image_grad, text_grad)


def solution(mesh):
    split = Mesh(mesh.devices.reshape(2, 4, LINE_Z, 2, mesh.shape["rep"]), BATCH_REP)
    return jax.shard_map(
        parts,
        mesh=split,
        in_specs=(P(BATCH, None), P(BATCH_REP, None), P()),
        out_specs=(P(), P(BATCH_REP, None), P(BATCH_REP, None)),
        check_vma=False,
    )
```

```python
import jax
import jax.numpy as jnp
from jax import lax
from jax.experimental import pallas as pl
from jax.experimental.pallas import tpu as pltpu
from jax.sharding import Mesh
from jax.sharding import PartitionSpec as P


BATCH = ("xh", "y", "z", "c")
BATCH_REP = ("xh", "y", "z", "c", "xl")
PLANE = ("xh", "y", "xl")
LINE = ("z", "c")
WIRE_SCALE = 8.0
VMEM_LIMIT = 24 * 1024 * 1024
ROWS = 64
LINE_Z = 8
PLANE_N = 16
HALF = LINE_Z * ROWS
BLOCK = 2 * HALF
LANES = 128
TILES = BLOCK // LANES
STEP = 256
FAR_FIRST = (4, 3, 5, 2, 6, 1, 7)
NT = (((1,), (1,)), ((), ()))
NN = (((1,), (0,)), ((), ()))
TN = (((0,), (0,)), ((), ()))


def exchanged(message, axis):
    return lax.all_to_all(message, axis, 0, 0, tiled=True)


def shifted(array, by):
    return lax.ppermute(array, "z", [(k, (k + by) % LINE_Z) for k in range(LINE_Z)])


def across(array, bit):
    return lax.ppermute(array, "z", [(k, k ^ bit) for k in range(LINE_Z)])


def swapped(array):
    return lax.ppermute(array, "c", [(0, 1), (1, 0)])


def as_column(line):
    return jnp.transpose(jnp.broadcast_to(line, (LANES, LANES)))[:ROWS, :1]


def as_line(column):
    return jnp.transpose(jnp.broadcast_to(column, (LANES, LANES)))[:1]


def placed(slots, pos):
    lanes = lax.broadcasted_iota(jnp.int32, (LINE_Z, LANES), 1)
    both = jnp.where(lanes < ROWS, slots[:LINE_Z], pltpu.roll(slots[LINE_Z:], ROWS, 1))
    return pltpu.roll(jnp.where(pos[0] == 0, both, pltpu.roll(both, ROWS, 1)), pos[1], 0)


def relative(both, pos):
    both = pltpu.roll(both, lax.rem(LINE_Z - pos[1], LINE_Z), 0)
    turned = pltpu.roll(both, ROWS, 1)
    same = pos[0] == 0
    return jnp.concatenate(
        [jnp.where(same, both, turned), jnp.where(same, turned, both)], axis=0
    )


def scores_kernel(pos, scale, own_text, text, *refs):
    blocks, rest = refs[: 2 * LINE_Z], refs[2 * LINE_Z :]
    scores, image, row_message, col_part, diag_part = rest
    for k in range(2 * LINE_Z):
        image[k * ROWS : (k + 1) * ROWS, :] = blocks[k][...]
    scale_value = scale[0]
    diag = scale_value * jnp.sum(
        blocks[0][...].astype(jnp.float32) * own_text[...].astype(jnp.float32)
    )
    text_rows = text[...]
    col_max = col_sum = None
    lines = []
    for i in range(BLOCK // STEP):
        span = slice(i * STEP, (i + 1) * STEP)
        part = scale_value * lax.dot_general(
            image[span, :], text_rows, NT, preferred_element_type=jnp.float32
        )
        scores[span, :] = part
        biggest = jnp.max(part, axis=1, keepdims=True)
        lse = biggest + jnp.log(jnp.sum(jnp.exp(part - biggest), axis=1, keepdims=True))
        for t in range(STEP // LANES):
            line = as_line(lse[t * LANES : (t + 1) * LANES])
            lines += [line, pltpu.roll(line, ROWS, 1)]
        top = jnp.max(part, axis=0, keepdims=True)
        new = top if i == 0 else jnp.maximum(col_max, top)
        total = jnp.sum(jnp.exp(part - new), axis=0, keepdims=True)
        col_sum = total if i == 0 else col_sum * jnp.exp(col_max - new) + total
        col_max = new
    message = placed(jnp.concatenate(lines, axis=0), pos)
    diag_part[...] = jnp.full(diag_part.shape, diag)
    row_message[...] = jnp.broadcast_to(message[None], row_message.shape)
    col_lse = col_max + jnp.log(col_sum)
    for i in range(TILES):
        col_part[i : i + 1, :] = col_lse[:, i * LANES : (i + 1) * LANES]


def joined(stats):
    biggest = jnp.max(stats, axis=0)
    return biggest + jnp.log(jnp.sum(jnp.exp(stats - biggest[None]), axis=0))


def rows_kernel(pos, heard, col_part, diag_part, row_lse, col_message):
    lse = joined(heard[...])
    row_lse[...] = relative(lse, pos)
    extra = lax.broadcasted_iota(jnp.int32, (TILES, LANES), 0)
    extra = jnp.where(extra == 0, jnp.sum(lse), diag_part[...])
    message = jnp.concatenate([col_part[...], extra], axis=0)
    col_message[...] = jnp.broadcast_to(message[None], col_message.shape)


def weights_kernel(
    pos, scores, row_lse, heard, text, weights, near, other_out, loss_part, rows_loss, other, sems
):
    col_lse = joined(heard[:, :TILES, :])
    extra = jnp.sum(heard[:, TILES:, :], axis=0)
    rows_loss[...] = jnp.broadcast_to(extra[:1], rows_loss.shape)
    loss_part[...] = jnp.sum(col_lse) - 2.0 * jnp.broadcast_to(extra[1:2], loss_part.shape)
    col_line = jnp.concatenate([col_lse[i : i + 1] for i in range(TILES)], axis=1)
    text_rows = text[...]
    copies = []
    half_steps = HALF // STEP
    for step in [*range(half_steps, 2 * half_steps), *range(half_steps)]:
        blocks = []
        for k in range(STEP // ROWS * step, STEP // ROWS * (step + 1)):
            part = scores[k * ROWS : (k + 1) * ROWS, :]
            both = jnp.exp(part - as_column(row_lse[k : k + 1, :])) + jnp.exp(part - col_line)
            if k == 0:
                row_ids = lax.broadcasted_iota(jnp.int32, part.shape, 0)
                column_ids = lax.broadcasted_iota(jnp.int32, part.shape, 1) - pos[2] * ROWS
                both = both - 2.0 * (row_ids == column_ids).astype(jnp.float32)
            blocks.append(both.astype(jnp.bfloat16))
        rows = jnp.concatenate(blocks, axis=0)
        weights[step * STEP : (step + 1) * STEP, :] = rows
        out = WIRE_SCALE * lax.dot_general(rows, text_rows, NN, preferred_element_type=jnp.float32)
        span = slice(step % half_steps * STEP, (step % half_steps + 1) * STEP)
        if step < half_steps:
            near[span, :] = out
        else:
            other[span, :] = out
            copies.append(
                pltpu.make_async_copy(other.at[span, :], other_out.at[span, :], sems.at[len(copies)])
            )
            copies[-1].start()
    for copy in copies:
        copy.wait()


def call(kernel, outs, spec, *args, out_spec=None, scratch=()):
    kinds = {
        "v": pl.BlockSpec(memory_space=pltpu.VMEM),
        "s": pl.BlockSpec(memory_space=pltpu.SMEM),
        "a": pl.BlockSpec(memory_space=pl.ANY),
    }
    return pl.pallas_call(
        kernel,
        out_shape=[jax.ShapeDtypeStruct(*o) for o in outs],
        in_specs=[kinds[k] for k in spec],
        out_specs=[kinds[k] for k in out_spec or "v" * len(outs)],
        scratch_shapes=scratch,
        compiler_params=pltpu.CompilerParams(vmem_limit_bytes=VMEM_LIMIT),
    )(*args)


def parts(image_embed, text_embed, logit_scale):
    f32, f16, bf16 = jnp.float32, jnp.float16, jnp.bfloat16
    width = text_embed.shape[1]
    pos = jnp.stack(
        [lax.axis_index("c"), lax.axis_index("z"), lax.axis_index(PLANE)]
    ).astype(jnp.int32)
    own_image = lax.dynamic_slice_in_dim(image_embed, lax.axis_index("xl") * ROWS, ROWS, 0)

    text_all = exchanged(
        jnp.broadcast_to(text_embed[None], (PLANE_N, ROWS, width)), PLANE
    ).reshape(BLOCK, width)
    near = [own_image] + [None] * (LINE_Z - 1)
    for k in FAR_FIRST:
        near[k] = shifted(own_image, -k)
    far = []
    for block in near:
        far.append(swapped(block))

    message = (PLANE_N, 2 * TILES, LANES)
    scores, image_all, row_message, col_part, diag_part = call(
        scores_kernel,
        [
            ((BLOCK, BLOCK), f32),
            ((BLOCK, width), bf16),
            ((PLANE_N, TILES, LANES), f32),
            ((TILES, LANES), f32),
            ((TILES, LANES), f32),
        ],
        "ss" + "v" * (2 + 2 * LINE_Z),
        pos, logit_scale, text_embed, text_all, *near, *far,
    )
    row_lse, col_message = call(
        rows_kernel,
        [((2 * LINE_Z, LANES), f32), (message, f32)],
        "svvv",
        pos, exchanged(row_message, LINE), col_part, diag_part,
    )
    weights, near_part, other_part, loss_sum, rows_loss = call(
        weights_kernel,
        [
            ((BLOCK, BLOCK), bf16),
            ((HALF, width), f32),
            ((HALF, width), f32),
            ((TILES, LANES), f32),
            ((TILES, LANES), f32),
        ],
        "svvvv",
        pos, scores, row_lse, exchanged(col_message, PLANE), text_all,
        out_spec="vvavv",
        scratch=[pltpu.VMEM((HALF, width), f32), pltpu.SemaphoreType.DMA((HALF // STEP,))],
    )
    arrived = swapped(other_part)
    loss_sum = loss_sum + swapped(loss_sum)
    loss_sum = loss_sum + across(loss_sum, 1)
    apart = {}
    for bits in (4, 2, 6):
        apart[bits] = across(loss_sum, bits)
    loss_sum = (loss_sum + apart[4]) + (apart[2] + apart[6])
    mean_loss = ((rows_loss + loss_sum) * (1.0 / (2 * ROWS * 256)))[0, 0]

    text_part = lax.dot_general(weights, image_all, TN, preferred_element_type=f32)
    text_part = (WIRE_SCALE * text_part).astype(f16).reshape(PLANE_N, ROWS, width)
    text_back = exchanged(text_part, PLANE)
    factor = logit_scale[0] * (0.5 / WIRE_SCALE)
    image_part = [
        near_part[k * ROWS : (k + 1) * ROWS] + arrived[k * ROWS : (k + 1) * ROWS]
        for k in range(LINE_Z)
    ]
    leaving = [part.astype(f16) for part in image_part]
    back = {}
    for k in FAR_FIRST:
        back[k] = shifted(leaving[k], k)
    text_sum = text_back[0].astype(f32)
    for k in range(1, PLANE_N):
        text_sum = text_sum + text_back[k].astype(f32)
    text_grad = factor * text_sum
    image_sum = image_part[0]
    for k in FAR_FIRST[:5]:
        image_sum = image_sum + back[k].astype(f32)
    image_sum = lax.optimization_barrier(image_sum)
    for k in FAR_FIRST[5:]:
        image_sum = image_sum + back[k].astype(f32)
    image_grad = factor * image_sum
    return (mean_loss, image_grad, text_grad)


def solution(mesh):
    split = Mesh(mesh.devices.reshape(2, 4, LINE_Z, 2, mesh.shape["rep"]), BATCH_REP)
    return jax.shard_map(
        parts,
        mesh=split,
        in_specs=(P(BATCH, None), P(BATCH_REP, None), P()),
        out_specs=(P(), P(BATCH_REP, None), P(BATCH_REP, None)),
        check_vma=False,
    )
```
